256 devices in a mesh: grp: 8 (over y_lo, x), mem: 32 (over z, y_hi, core).
Axes of the slice: x: 4, y: 4 (y_hi: 2, y_lo: 2; y = y_hi * 2 + y_lo), z: 8, core: 2. Of those that a mesh axis runs over, the one named last changes fastest.
Arguments:
- factors: bfloat16 [256, 512, 2048], P(('grp', 'mem')), may hold values from -1 to 1
- occ_energy: bfloat16 [256], P(('grp', 'mem')), may hold values from -1.5 to -0.29882812
- vir_energy: bfloat16 [512], replicated, may hold values from 0.3984375 to 3
- pair_code: int32 [8, 32, 3], P('grp'), may hold values from 0 to 2
- pair_count: int32 [8, 32], P('grp'), may hold values from 1 to 3
Outputs:
- aux_density: bfloat16 [256, 512, 2048], P(('grp', 'mem'))
- lagrangian: bfloat16 [256, 512, 2048], P(('grp', 'mem'))
The draws below stay inside these ranges and needn't reach their ends.
Inputs may be any that keep to these rules, and one draw needn't show every extreme that they name: `pair_code`: only the first pair_count entries of a device's list are read; entries may repeat.
All inputs are finite; a program needn't handle non-finite values.
Results may differ from the reference program's by a relative error of at most 0.0056.
Values may be sent and summed in bfloat16 or wider, within the bound.
A program may use at most 128 MiB of HBM per device.

```python
import jax
import jax.numpy as jnp
from jax import lax

V = 512
A = 2048
OCC_DEV = 1
SLOTS = 3
ROUNDS = 2
OCC = 256
N_GRP = 8
N_MEM = 32


def draw_factors(key, part):
    unit_scale = A ** (-0.25)
    own_part = jax.random.normal(key, (OCC, V, A), jnp.float32)
    values_all = own_part
    return jnp.clip(values_all * unit_scale, -1.0, 1.0).astype(jnp.bfloat16)


def plant(drawn, stream_key, smallest, largest):
    longest = drawn.shape.index(max(drawn.shape))
    spots = []
    for shift in (0, 1):
        where = [jax.random.randint(jax.random.fold_in(stream_key, axis), (), 0, length) for axis, length in enumerate(drawn.shape)]
        where[longest] = (where[longest] + shift) % drawn.shape[longest]
        spots.append(tuple(where))
    return drawn.at[spots[0]].set(smallest).at[spots[1]].set(largest)


def block_levels(rng, shape, cuts, least, top_value):
    def one(dim, shards_of):
        steps = jax.random.uniform(jax.random.fold_in(jax.random.fold_in(rng, 6), dim), (shards_of,), jnp.float32, least / len(cuts), top_value / len(cuts))
        return jnp.repeat(jnp.exp(steps), shape[dim] // shards_of).reshape((-1,) + (1,) * (len(shape) - dim - 1))

    factor_of = one(*cuts[0])
    for cut in cuts[1:]:
        factor_of = factor_of * one(*cut)
    return factor_of


def setup_inputs(seed: int = 0) -> dict:
    key_of = jax.random.split(jax.random.key(seed), 6)
    return {
        "factors": draw_factors(jax.random.fold_in(key_of[5], 71), 0),
        "occ_energy": jnp.clip(-1.5 + 1.2011719 * jax.random.uniform(key_of[1], (OCC,), jnp.float32) ** block_levels(key_of[1], (OCC,), ((0, 256),), -0.2, 0.2), -1.5, -0.29882812).astype(jnp.bfloat16),
        "vir_energy": jnp.clip(jax.random.uniform(key_of[2], (V,), jnp.float32, 0.3984375, 3.0), 0.3984375, 3.0).astype(jnp.bfloat16),
        "pair_code": plant(jax.random.randint(key_of[3], (N_GRP, N_MEM, SLOTS), 0, (ROUNDS + 1) * OCC_DEV * OCC_DEV), jax.random.fold_in(key_of[3], 1), 0, ((ROUNDS + 1) * OCC_DEV * OCC_DEV) - 1).astype(jnp.int32),
        "pair_count": plant(jax.random.randint(key_of[4], (N_GRP, N_MEM), 1, SLOTS + 1), jax.random.fold_in(key_of[4], 1), 1, SLOTS).astype(jnp.int32),
    }


def decode_pair(code):
    round_no = code // (OCC_DEV * OCC_DEV)
    left_orb = (code // OCC_DEV) % OCC_DEV
    right_orb = code % OCC_DEV
    return round_no, left_orb, right_orb


def add_at(target, indices, contribution):
    zero_index = jnp.zeros((), jnp.int32)
    anchor = tuple(indices) + (zero_index,) * contribution.ndim
    extent = (1,) * len(indices) + contribution.shape
    current = lax.dynamic_slice(target, anchor, extent)
    return lax.dynamic_update_slice(target, current + contribution.reshape(extent), anchor)


def reference(factors, occ_energy, vir_energy, pair_code, pair_count):
    virtual = vir_energy.astype(jnp.float32)
    group_span = N_MEM * OCC_DEV

    def group_work(group_no):
        group_factors = lax.dynamic_slice_in_dim(factors, group_no * group_span, group_span, 0).reshape(N_MEM, OCC_DEV, V, A)
        group_energy = lax.dynamic_slice_in_dim(occ_energy, group_no * group_span, group_span, 0).reshape(N_MEM, OCC_DEV).astype(jnp.float32)
        group_codes = lax.dynamic_index_in_dim(pair_code, group_no, 0, keepdims=False)
        group_counts = lax.dynamic_index_in_dim(pair_count, group_no, 0, keepdims=False)

        def device_work(carry_in, member):
            def pair_step(slot_no, carry_pair):
                density, gamma_all = carry_pair
                round_no, left_orb, right_orb = decode_pair(group_codes[member, slot_no])
                shift_bits = jnp.left_shift(jnp.int32(1), jnp.maximum(round_no - 1, 0))
                partner = jnp.where(round_no == 0, member, jnp.bitwise_xor(member, shift_bits)).astype(jnp.int32)
                left_block = group_factors[member, left_orb]
                right_block = group_factors[partner, right_orb]
                integrals = lax.dot_general(left_block, right_block, (((1,), (1,)), ((), ())), preferred_element_type=jnp.float32)
                denominator = virtual[:, None] + virtual[None, :] - group_energy[member, left_orb] - group_energy[partner, right_orb]
                amp_tile = (integrals / denominator).astype(jnp.bfloat16)
                density = density + lax.dot_general(amp_tile, amp_tile, (((1,), (1,)), ((), ())), preferred_element_type=jnp.float32)
                near_term = jnp.dot(amp_tile, right_block, preferred_element_type=jnp.float32)
                far_term = lax.dot_general(amp_tile, left_block, (((0,), (0,)), ((), ())), preferred_element_type=jnp.float32)
                gamma_all = add_at(gamma_all, (member, left_orb), near_term)
                gamma_all = add_at(gamma_all, (partner, right_orb), far_term)
                return density, gamma_all

            return lax.fori_loop(0, group_counts[member], pair_step, carry_in), None

        initial = (jnp.zeros((V, V), jnp.float32), jnp.zeros((N_MEM, OCC_DEV, V, A), jnp.float32))
        (density, gamma_all), _ = lax.scan(device_work, initial, jnp.arange(N_MEM, dtype=jnp.int32))
        return density, gamma_all.astype(jnp.bfloat16).reshape(group_span, V, A)

    densities, gammas = lax.map(group_work, jnp.arange(N_GRP, dtype=jnp.int32))
    density = jnp.sum(densities, axis=0)
    density_tile = (density * (1.0 / (8.0 * N_GRP * N_MEM))).astype(jnp.bfloat16)
    aux_density = gammas.reshape(OCC, V, A)

    def apply_density(block):
        product = lax.dot_general(density_tile, block, (((1,), (1,)), ((), ())), preferred_element_type=jnp.float32)
        return jnp.transpose(product, (1, 0, 2)).astype(jnp.bfloat16)

    lagrangian = lax.map(apply_density, factors.reshape(N_GRP, group_span, V, A)).reshape(OCC, V, A)
    return aux_density, lagrangian
```

```python
import functools

import jax
import jax.numpy as jnp
from jax import lax
from jax.experimental import pallas as pl
from jax.experimental.pallas import tpu as pltpu
from jax.sharding import PartitionSpec as P

MESH = pl.DeviceIdType.MESH
NX, NY, NZ = 4, 4, 8
CHUNKS = 16
FIRST = 7
LEAD = 2
F32, BF16 = jnp.float32, jnp.bfloat16


def nt(a, b):
    return lax.dot_general(a, b, (((1,), (1,)), ((), ())), preferred_element_type=F32)


def tn(a, b):
    return lax.dot_general(a, b, (((0,), (0,)), ((), ())), preferred_element_type=F32)


def nn(a, b):
    return jnp.dot(a, b, preferred_element_type=F32)


def body(
    b_own, table, code, count,
    gamma_out, lag_out,
    ball, tall, ens, vsum, acc, dens, dl_send, dl_recv, xs, xr, zs, zr, ys, yr, dfull,
    pair_s, pair_r, bulk_s, bulk_r, en_s, en_r, dl_s, dl_rs,
    x_s, x_r, z_s, z_r, y_s, y_r, za_s, za_r, xa_s, xa_r, fw_s, fw_r,
):
    V, A = b_own.shape
    g, m = lax.axis_index("grp"), lax.axis_index("mem")
    x, ylo = lax.rem(g, NX), g // NX
    core, yhi, z = lax.rem(m, 2), lax.rem(m // 2, 2), m // 4
    y = yhi * 2 + ylo
    mate = m + 1 - 2 * core
    far = m + 2 - 4 * yhi
    early = core == yhi
    late = core != yhi
    rows_x, rows_z = V // NX, V // NX // NZ

    def to_x(d):
        return {"grp": ylo * NX + lax.rem(x + d, NX), "mem": m}

    def to_z(d):
        return {"grp": g, "mem": lax.rem(z + d, NZ) * 4 + yhi * 2 + core}

    def to_y(d):
        other = lax.rem(y + d, NY)
        hi, lo = other // 2, lax.rem(other, 2)
        return {"grp": lo * NX + x, "mem": z * 4 + hi * 3}

    to_mate = {"grp": g, "mem": mate}
    to_far = {"grp": g, "mem": far}

    barrier = pltpu.get_barrier_semaphore()

    def greet(where):
        pl.semaphore_signal(barrier, inc=1, device_id=where, device_id_type=MESH)

    def remote(src, dst, send, recv, where):
        return pltpu.make_async_remote_copy(
            src_ref=src, dst_ref=dst, send_sem=send, recv_sem=recv, device_id=where, device_id_type=MESH
        )

    greet(to_mate)
    greet(to_far)

    @pl.when(early)
    def _():
        for d in range(1, NX):
            greet(to_x(d))
        for d in range(1, NZ):
            greet(to_z(d))
        for d in range(1, NY):
            greet(to_y(d))

    crows = V // CHUNKS

    def bulk(i):
        r = pl.ds(pl.multiple_of(i * crows, crows), crows)
        return remote(b_own.at[r], ball.at[1, r], bulk_s.at[i], bulk_r.at[i], to_far)

    def bulk_start(lo, hi):
        @pl.loop(lo, hi)
        def _(i):
            bulk(i).start()

    def bulk_wait(lo, hi):
        @pl.loop(lo, hi)
        def _(i):
            bulk(i).wait_recv()

    pair = remote(b_own, ball.at[0], pair_s, pair_r, to_mate)
    en1 = remote(table.at[8:16], ens.at[0], en_s.at[0], en_r.at[0], to_mate)
    en2 = remote(table.at[8:16], ens.at[1], en_s.at[1], en_r.at[1], to_far)

    @pl.when(late)
    def _():
        pl.semaphore_wait(barrier, 2)

    @pl.when(early)
    def _():
        pl.semaphore_wait(barrier, 2 + NX - 1 + NZ - 1 + NY - 1)

    en1.start()
    en2.start()

    @pl.when(late)
    def _():
        bulk_start(0, CHUNKS)

    pair.start()

    def lives(who, rnd):
        total = jnp.int32(0)
        for s in range(code.shape[2]):
            hit = jnp.logical_and(code[0, who, s] == rnd, s < count[0, who])
            total = total + jnp.where(hit, 1, 0)
        return total.astype(F32)

    c0, c1, c2 = lives(m, 0), lives(m, 1), lives(m, 2)
    d1, d2 = lives(mate, 1), lives(far, 2)

    for i in range(V // 128):
        column = jnp.broadcast_to(table[0:1, i * 128 : (i + 1) * 128], (128, 128)).T
        for j in range(V // 128):
            vsum[i * 128 : (i + 1) * 128, j * 128 : (j + 1) * 128] = column + table[0:1, j * 128 : (j + 1) * 128]

    acc[...] = jnp.zeros_like(acc)
    dens[...] = jnp.zeros_like(dens)
    own = table[8:9, 0:1]
    blocks = (b_own, ball.at[0], ball.at[1])

    def tile(r, lo, width, other):
        cols = pl.ds(pl.multiple_of(lo, 128), width)
        k = nt(b_own[...], blocks[r][cols, :])
        denominator = vsum[:, cols] - own - other
        tall[r, :, cols] = (k / denominator).astype(BF16)

    def gamma(r, lo, width, weight):
        rows = pl.ds(pl.multiple_of(lo, 128), width)

        @pl.loop(0, A // 256)
        def _(p):
            c = pl.ds(pl.multiple_of(p * 256, 256), 256)
            acc[:, c] = acc[:, c] + weight * nn(tall[r, :, rows], blocks[r][rows, c])

    def outer(r, lo, width, weight):
        cols = pl.ds(pl.multiple_of(lo, 128), width)

        @pl.loop(0, V // 256)
        def _(p):
            c = pl.ds(pl.multiple_of(p * 256, 256), 256)
            dens[:, c] = dens[:, c] + weight * nt(tall[r, :, cols], tall[r, c, cols])

    def inner(r, weight):
        @pl.loop(0, V // 256)
        def _(p):
            c = pl.ds(pl.multiple_of(p * 256, 256), 256)
            dens[:, c] = dens[:, c] + weight * tn(tall[r], tall[r, :, c])

    def whole(r, other, outer_weight, gamma_weight):
        @pl.loop(0, V // 256)
        def _(p):
            tile(r, p * 256, 256, other)

        outer(r, 0, V, outer_weight)
        gamma(r, 0, V, gamma_weight)

    whole(0, own, c0, c0 + c0)
    en1.wait_recv()
    pair.wait_recv()
    whole(1, ens[0, 0:1, 0:1], c1, c1 + d1)

    dl = remote(dl_send, dl_recv, dl_s, dl_rs, to_mate)

    @pl.when(late)
    def _():
        dl_send[...] = dens[...].astype(BF16)
        dl.start()

    en2.wait_recv()
    w2 = c2 + d2
    far_energy = ens[1, 0:1, 0:1]

    bulk_wait(0, CHUNKS // 2)
    tile(2, 0, 256, far_energy)

    @pl.when(early)
    def _():
        outer(2, 0, 256, c2)

    gamma(2, 0, 256, w2)
    bulk_wait(CHUNKS // 2, 3 * CHUNKS // 4)
    tile(2, 256, 128, far_energy)

    @pl.when(early)
    def _():
        outer(2, 256, 128, c2)

    gamma(2, 256, 128, w2)
    bulk_wait(3 * CHUNKS // 4, CHUNKS - LEAD)

    @pl.when(early)
    def _():
        bulk_start(0, FIRST)

    bulk_wait(CHUNKS - LEAD, CHUNKS)
    tile(2, 384, 128, far_energy)

    def block_x(d):
        return pl.ds(pl.multiple_of(lax.rem(x + d, NX) * rows_x, rows_x), rows_x)

    def block_z(d):
        return pl.ds(pl.multiple_of(lax.rem(z + d, NZ) * rows_z, rows_z), rows_z)

    def piece(d):
        return pl.ds(pl.multiple_of(x * rows_x + lax.rem(z + d, NZ) * rows_z, rows_z), rows_z)

    x_order = (1, 3, 2)
    z_order = (4, 3, 5, 2, 6, 1, 7)

    @pl.when(early)
    def _():
        outer(2, 384, 128, c2)
        inner(2, d2)
        dl.wait_recv()
        dens[...] = dens[...] + dl_recv[...].astype(F32)
        xs[...] = dens[...].astype(BF16)
        for d in x_order:
            remote(xs.at[block_x(d)], xr.at[d - 1], x_s.at[d - 1], x_r.at[d - 1], to_x(d)).start()

    gamma(2, 384, 128, w2)
    gamma_out[...] = acc[...].astype(BF16)

    def x_copy(d):
        return remote(xs.at[block_x(d)], xr.at[d - 1], x_s.at[d - 1], x_r.at[d - 1], to_x(d))

    def z_copy(d):
        return remote(zs.at[block_z(d)], zr.at[d - 1], z_s.at[d - 1], z_r.at[d - 1], to_z(d))

    def y_copy(d):
        return remote(ys, yr.at[d - 1], y_s.at[d - 1], y_r.at[d - 1], to_y(d))

    def za_copy(d):
        return remote(dfull.at[piece(0)], dfull.at[piece(0)], za_s.at[d - 1], za_r.at[d - 1], to_z(d))

    def za_arrival(d):
        r = piece(NZ - d)
        return remote(dfull.at[r], dfull.at[r], za_s.at[d - 1], za_r.at[d - 1], to_z(d))

    def xa_copy(d):
        r = block_x(0)
        return remote(dfull.at[r], dfull.at[r], xa_s.at[d - 1], xa_r.at[d - 1], to_x(d))

    def xa_arrival(d):
        r = block_x(NX - d)
        return remote(dfull.at[r], dfull.at[r], xa_s.at[d - 1], xa_r.at[d - 1], to_x(d))

    def fw_copy(d):
        r = block_x(lax.rem(NX - d, NX))
        return remote(dfull.at[r], dfull.at[r], fw_s.at[d], fw_r.at[d], to_mate)

    def lag(d):
        r = block_x(lax.rem(NX - d, NX))

        @pl.loop(0, A // 512)
        def _(p):
            c = pl.ds(pl.multiple_of(p * 512, 512), 512)
            lag_out[r, c] = nn(dfull[r, :], b_own[:, c]).astype(BF16)

    @pl.when(early)
    def _():
        for d in x_order:
            x_copy(d).wait_recv()
        sum_x = dens[block_x(0), :]
        for d in range(NX - 1):
            sum_x = sum_x + xr[d].astype(F32)
        dens[0:rows_x, :] = sum_x
        zs[...] = sum_x.astype(BF16)
        for d in z_order:
            z_copy(d).start()
        for d in z_order:
            z_copy(d).wait_recv()
        sum_z = dens[block_z(0), :]
        for d in range(NZ - 1):
            sum_z = sum_z + zr[d].astype(F32)
        ys[...] = sum_z.astype(BF16)
        for d in (2, 1, 3):
            y_copy(d).start()
        bulk_start(FIRST, CHUNKS)
        for d in (2, 1, 3):
            y_copy(d).wait_recv()
        total = sum_z
        for d in range(NY - 1):
            total = total + yr[d].astype(F32)
        dfull[piece(0), :] = (total * (1.0 / (8.0 * 2 * NX * NY * NZ))).astype(BF16)
        for d in z_order:
            za_copy(d).start()
        for d in z_order:
            za_arrival(d).wait_recv()
        for d in x_order:
            xa_copy(d).start()
        fw_copy(0).start()
        lag(0)
        for d in x_order:
            xa_arrival(d).wait_recv()
            fw_copy(d).start()
            lag(d)

    @pl.when(late)
    def _():
        for d in (0,) + x_order:
            fw_copy(d).wait_recv()
            lag(d)

    en1.wait_send()
    en2.wait_send()
    pair.wait_send()

    @pl.loop(0, CHUNKS)
    def _(i):
        bulk(i).wait_send()

    @pl.when(late)
    def _():
        dl.wait_send()

    @pl.when(early)
    def _():
        for d in range(1, NX):
            x_copy(d).wait_send()
            xa_copy(d).wait_send()
        for d in range(1, NZ):
            z_copy(d).wait_send()
            za_copy(d).wait_send()
        for d in range(1, NY):
            y_copy(d).wait_send()
        for d in range(NX):
            fw_copy(d).wait_send()


def per_device(factors, occ_energy, vir_energy, pair_code, pair_count):
    _, V, A = factors.shape
    table = jnp.concatenate(
        [
            jnp.broadcast_to(vir_energy.astype(F32)[None, :], (8, V)),
            jnp.broadcast_to(occ_energy.astype(F32)[:, None], (8, V)),
        ]
    )
    dma = pltpu.SemaphoreType.DMA
    vmem, smem = pl.BlockSpec(memory_space=pltpu.VMEM), pl.BlockSpec(memory_space=pltpu.SMEM)
    rx, rz = V // NX, V // NX // NZ
    flops = 2 * V * V * A * 7
    aux, lag = pl.pallas_call(
        body,
        out_shape=[jax.ShapeDtypeStruct((V, A), BF16)] * 2,
        in_specs=[vmem, vmem, smem, smem],
        out_specs=[vmem, vmem],
        scratch_shapes=[
            pltpu.VMEM((2, V, A), BF16),
            pltpu.VMEM((3, V, V), BF16),
            pltpu.VMEM((2, 8, V), F32),
            pltpu.VMEM((V, V), F32),
            pltpu.VMEM((V, A), F32),
            pltpu.VMEM((V, V), F32),
            pltpu.VMEM((V, V), BF16),
            pltpu.VMEM((V, V), BF16),
            pltpu.VMEM((V, V), BF16),
            pltpu.VMEM((NX - 1, rx, V), BF16),
            pltpu.VMEM((rx, V), BF16),
            pltpu.VMEM((NZ - 1, rz, V), BF16),
            pltpu.VMEM((rz, V), BF16),
            pltpu.VMEM((NY - 1, rz, V), BF16),
            pltpu.VMEM((V, V), BF16),
            dma, dma, dma((CHUNKS,)), dma((CHUNKS,)), dma((2,)), dma((2,)), dma, dma,
            dma((NX - 1,)), dma((NX - 1,)), dma((NZ - 1,)), dma((NZ - 1,)), dma((NY - 1,)), dma((NY - 1,)),
            dma((NZ - 1,)), dma((NZ - 1,)), dma((NX - 1,)), dma((NX - 1,)), dma((NX,)), dma((NX,)),
        ],
        compiler_params=pltpu.CompilerParams(
            collective_id=0, has_side_effects=True, vmem_limit_bytes=36 * 2**20
        ),
        cost_estimate=pl.CostEstimate(flops=flops, bytes_accessed=8 * V * A, transcendentals=0),
        name="window",
    )(factors.reshape(V, A), table, pair_code, pair_count)
    return aux.reshape(1, V, A), lag.reshape(1, V, A)


def solution(mesh):
    in_specs = (
        P(("grp", "mem"), None, None),
        P(("grp", "mem")),
        P(),
        P("grp", None, None),
        P("grp", None),
    )
    out_specs = (P(("grp", "mem"), None, None), P(("grp", "mem"), None, None))
    return jax.shard_map(
        per_device, mesh=mesh, in_specs=in_specs, out_specs=out_specs, check_vma=False
    )
```

```python
import functools

import jax
import jax.numpy as jnp
from jax import lax
from jax.experimental import pallas as pl
from jax.experimental.pallas import tpu as pltpu
from jax.sharding import PartitionSpec as P

MESH = pl.DeviceIdType.MESH
NX, NY, NZ = 4, 4, 8
CHUNKS = 16
FIRST = 7
LEAD = 2
LAST = 384
FAR_FIRST = sorted(
    range(1, NX * NZ),
    key=lambda d: (-min(d // NZ, NX - d // NZ) - min(d % NZ, NZ - d % NZ), d),
)
F32, BF16 = jnp.float32, jnp.bfloat16


def nt(a, b):
    return lax.dot_general(a, b, (((1,), (1,)), ((), ())), preferred_element_type=F32)


def tn(a, b):
    return lax.dot_general(a, b, (((0,), (0,)), ((), ())), preferred_element_type=F32)


def nn(a, b):
    return jnp.dot(a, b, preferred_element_type=F32)


def body(
    b_hbm, table, code, count,
    gamma_out, lag_out,
    b_own, ball, tall, ens, vsum, acc, dens, dl_send, dl_recv, xs, pr, ys, yr, dfull,
    load_sem, pair_s, pair_r, bulk_s, bulk_r, en_s, en_r, dl_s, dl_rs,
    p_s, p_r, y_s, y_r, f_s, f_r, fw_s, fw_r,
):
    V, A = b_hbm.shape
    g, m = lax.axis_index("grp"), lax.axis_index("mem")
    x, ylo = lax.rem(g, NX), g // NX
    core, yhi, z = lax.rem(m, 2), lax.rem(m // 2, 2), m // 4
    y = yhi * 2 + ylo
    mate = m + 1 - 2 * core
    far = m + 2 - 4 * yhi
    early = core == yhi
    late = core != yhi
    rows_x, rows_z = V // NX, V // NX // NZ

    load = pltpu.make_async_copy(b_hbm, b_own, load_sem)
    load.start()

    def to_plane(d):
        dx, dz = d // NZ, d % NZ
        return {
            "grp": ylo * NX + lax.rem(x + dx, NX),
            "mem": lax.rem(z + dz, NZ) * 4 + yhi * 2 + core,
        }

    def to_y(d):
        other = lax.rem(y + d, NY)
        hi, lo = other // 2, lax.rem(other, 2)
        return {"grp": lo * NX + x, "mem": z * 4 + hi * 3}

    to_mate = {"grp": g, "mem": mate}
    to_far = {"grp": g, "mem": far}

    barrier = pltpu.get_barrier_semaphore()

    def greet(where):
        pl.semaphore_signal(barrier, inc=1, device_id=where, device_id_type=MESH)

    def remote(src, dst, send, recv, where):
        return pltpu.make_async_remote_copy(
            src_ref=src, dst_ref=dst, send_sem=send, recv_sem=recv, device_id=where, device_id_type=MESH
        )

    greet(to_mate)
    greet(to_far)

    @pl.when(early)
    def _():
        for d in FAR_FIRST:
            greet(to_plane(d))
        for d in range(1, NY):
            greet(to_y(d))

    crows = V // CHUNKS

    def bulk(i):
        r = pl.ds(pl.multiple_of(i * crows, crows), crows)
        return remote(b_own.at[r], ball.at[1, r], bulk_s.at[i], bulk_r.at[i], to_far)

    def bulk_start(lo, hi):
        @pl.loop(lo, hi)
        def _(i):
            bulk(i).start()

    def bulk_wait(lo, hi):
        @pl.loop(lo, hi)
        def _(i):
            bulk(i).wait_recv()

    pair = remote(b_own, ball.at[0], pair_s, pair_r, to_mate)
    en1 = remote(table.at[8:16], ens.at[0], en_s.at[0], en_r.at[0], to_mate)
    en2 = remote(table.at[8:16], ens.at[1], en_s.at[1], en_r.at[1], to_far)

    @pl.when(late)
    def _():
        pl.semaphore_wait(barrier, 2)

    @pl.when(early)
    def _():
        pl.semaphore_wait(barrier, 2 + NX * NZ - 1 + NY - 1)

    en1.start()
    en2.start()
    load.wait()

    @pl.when(late)
    def _():
        bulk_start(0, CHUNKS)

    pair.start()

    def lives(who, rnd):
        total = jnp.int32(0)
        for s in range(code.shape[0]):
            hit = jnp.logical_and(code[s, 0, who] == rnd, s < count[0, who])
            total = total + jnp.where(hit, 1, 0)
        return total.astype(F32)

    c0, c1, c2 = lives(m, 0), lives(m, 1), lives(m, 2)
    d1, d2 = lives(mate, 1), lives(far, 2)

    for i in range(V // 128):
        column = jnp.broadcast_to(table[0:1, i * 128 : (i + 1) * 128], (128, 128)).T
        for j in range(V // 128):
            vsum[i * 128 : (i + 1) * 128, j * 128 : (j + 1) * 128] = column + table[0:1, j * 128 : (j + 1) * 128]

    acc[...] = jnp.zeros_like(acc)
    dens[...] = jnp.zeros_like(dens)
    own = table[8:9, 0:1]
    blocks = (b_own, ball.at[0], ball.at[1])

    def tile(r, lo, width, other):
        cols = pl.ds(pl.multiple_of(lo, 128), width)
        k = nt(b_own[...], blocks[r][cols, :])
        denominator = vsum[:, cols] - own - other
        tall[r, :, cols] = (k / denominator).astype(BF16)

    def gamma(r, lo, width, weight):
        rows = pl.ds(pl.multiple_of(lo, 128), width)

        @pl.loop(0, A // 256)
        def _(p):
            c = pl.ds(pl.multiple_of(p * 256, 256), 256)
            acc[:, c] = acc[:, c] + weight * nn(tall[r, :, rows], blocks[r][rows, c])

    def outer(r, lo, width, weight):
        cols = pl.ds(pl.multiple_of(lo, 128), width)

        @pl.loop(0, V // 256)
        def _(p):
            c = pl.ds(pl.multiple_of(p * 256, 256), 256)
            dens[:, c] = dens[:, c] + weight * nt(tall[r, :, cols], tall[r, c, cols])

    def inner(r, weight):
        @pl.loop(0, V // 256)
        def _(p):
            c = pl.ds(pl.multiple_of(p * 256, 256), 256)
            dens[:, c] = dens[:, c] + weight * tn(tall[r], tall[r, :, c])

    def whole(r, other, outer_weight, gamma_weight):
        @pl.loop(0, V // 256)
        def _(p):
            tile(r, p * 256, 256, other)

        outer(r, 0, V, outer_weight)
        gamma(r, 0, V, gamma_weight)

    whole(0, own, c0, c0 + c0)
    en1.wait_recv()
    pair.wait_recv()
    whole(1, ens[0, 0:1, 0:1], c1, c1 + d1)

    dl = remote(dl_send, dl_recv, dl_s, dl_rs, to_mate)

    @pl.when(late)
    def _():
        dl_send[...] = dens[...].astype(BF16)
        dl.start()

    en2.wait_recv()
    w2 = c2 + d2
    far_energy = ens[1, 0:1, 0:1]

    bulk_wait(0, CHUNKS // 2)
    tile(2, 0, 256, far_energy)

    @pl.when(early)
    def _():
        outer(2, 0, 256, c2)

    gamma(2, 0, 256, w2)
    bulk_wait(CHUNKS // 2, 3 * CHUNKS // 4)
    tile(2, 256, 128, far_energy)

    @pl.when(early)
    def _():
        outer(2, 256, 128, c2)

    gamma(2, 256, 128, w2)
    @pl.when(early)
    def _():
        dl.wait_recv()

        @pl.loop(0, V // 256)
        def _(p):
            c = pl.ds(pl.multiple_of(p * 256, 256), 256)
            dens[:, c] = dens[:, c] + dl_recv[:, c].astype(F32)

        for lo in (0, 128, 256):
            rows = slice(lo, lo + 128)
            dens[rows, 0:LAST] = dens[rows, 0:LAST] + d2 * tn(tall[2, :, rows], tall[2, :, 0:LAST])

    bulk_wait(3 * CHUNKS // 4, CHUNKS - LEAD)

    @pl.when(early)
    def _():
        bulk_start(0, FIRST)

    bulk_wait(CHUNKS - LEAD, CHUNKS)
    tile(2, LAST, 128, far_energy)

    def piece(d):
        dx, dz = d // NZ, d % NZ
        return pl.ds(
            pl.multiple_of(lax.rem(x + dx, NX) * rows_x + lax.rem(z + dz, NZ) * rows_z, rows_z), rows_z
        )

    def back(d):
        dx, dz = d // NZ, d % NZ
        return ((NX - dx) % NX) * NZ + (NZ - dz) % NZ

    def block_x(d):
        return pl.ds(pl.multiple_of(lax.rem(x + d, NX) * rows_x, rows_x), rows_x)

    def part_copy(d):
        return remote(xs.at[piece(d)], pr.at[d - 1], p_s.at[d - 1], p_r.at[d - 1], to_plane(d))

    def y_copy(d):
        return remote(ys, yr.at[d - 1], y_s.at[d - 1], y_r.at[d - 1], to_y(d))

    def full_copy(d):
        r = piece(0)
        return remote(dfull.at[r], dfull.at[r], f_s.at[d - 1], f_r.at[d - 1], to_plane(d))

    def full_arrival(d):
        r = piece(back(d))
        return remote(dfull.at[r], dfull.at[r], f_s.at[d - 1], f_r.at[d - 1], to_plane(d))

    def fw_copy(d):
        r = block_x((NX - d) % NX)
        return remote(dfull.at[r], dfull.at[r], fw_s.at[d], fw_r.at[d], to_mate)

    def lag(d):
        r = block_x((NX - d) % NX)

        @pl.loop(0, A // 512)
        def _(p):
            c = pl.ds(pl.multiple_of(p * 512, 512), 512)
            lag_out[r, c] = nn(dfull[r, :], b_own[:, c]).astype(BF16)

    x_order = (0, 1, 3, 2)

    @pl.when(early)
    def _():
        new = tall[2, :, LAST:V]
        dens[0:LAST, LAST:V] = dens[0:LAST, LAST:V] + d2 * tn(tall[2, :, 0:LAST], new)
        dens[LAST:V, :] = dens[LAST:V, :] + d2 * tn(new, tall[2])

        @pl.loop(0, V // 256)
        def _(p):
            c = pl.ds(pl.multiple_of(p * 256, 256), 256)
            total = dens[:, c] + c2 * nt(new, tall[2, c, LAST:V])
            dens[:, c] = total
            xs[:, c] = total.astype(BF16)

        for d in FAR_FIRST:
            part_copy(d).start()

    gamma(2, LAST, 128, w2)
    gamma_out[...] = acc[...].astype(BF16)

    @pl.when(early)
    def _():
        total = dens[piece(0), :]
        for d in FAR_FIRST[::-1]:
            part_copy(d).wait_recv()
            total = total + pr[d - 1].astype(F32)
        ys[...] = total.astype(BF16)
        for d in (2, 1, 3):
            y_copy(d).start()
        bulk_start(FIRST, CHUNKS)
        for d in (1, 3, 2):
            y_copy(d).wait_recv()
            total = total + yr[d - 1].astype(F32)
        dfull[piece(0), :] = (total * (1.0 / (8.0 * 2 * NX * NY * NZ))).astype(BF16)
        for d in FAR_FIRST:
            full_copy(d).start()
        for dx in x_order:
            for dz in (0, 1, 7, 2, 6, 3, 5, 4):
                if dx or dz:
                    full_arrival(dx * NZ + dz).wait_recv()
            fw_copy(dx).start()
            lag(dx)

    @pl.when(late)
    def _():
        for dx in x_order:
            fw_copy(dx).wait_recv()
            lag(dx)

    en1.wait_send()
    en2.wait_send()
    pair.wait_send()

    @pl.loop(0, CHUNKS)
    def _(i):
        bulk(i).wait_send()

    @pl.when(late)
    def _():
        dl.wait_send()

    @pl.when(early)
    def _():
        for d in range(1, NX * NZ):
            part_copy(d).wait_send()
            full_copy(d).wait_send()
        for d in range(1, NY):
            y_copy(d).wait_send()
        for d in range(NX):
            fw_copy(d).wait_send()


def per_device(factors, occ_energy, vir_energy, pair_code, pair_count):
    _, V, A = factors.shape
    table = jnp.concatenate(
        [
            jnp.broadcast_to(vir_energy.astype(F32)[None, :], (8, V)),
            jnp.broadcast_to(occ_energy.astype(F32)[:, None], (8, V)),
        ]
    )
    dma = pltpu.SemaphoreType.DMA
    vmem, smem = pl.BlockSpec(memory_space=pltpu.VMEM), pl.BlockSpec(memory_space=pltpu.SMEM)
    rz, plane = V // NX // NZ, NX * NZ - 1
    flops = 2 * V * V * A * 7
    aux, lag = pl.pallas_call(
        body,
        out_shape=[jax.ShapeDtypeStruct((V, A), BF16)] * 2,
        in_specs=[pl.BlockSpec(memory_space=pltpu.HBM), vmem, smem, smem],
        out_specs=[vmem, vmem],
        scratch_shapes=[
            pltpu.VMEM((V, A), BF16),
            pltpu.VMEM((2, V, A), BF16),
            pltpu.VMEM((3, V, V), BF16),
            pltpu.VMEM((2, 8, V), F32),
            pltpu.VMEM((V, V), F32),
            pltpu.VMEM((V, A), F32),
            pltpu.VMEM((V, V), F32),
            pltpu.VMEM((V, V), BF16),
            pltpu.VMEM((V, V), BF16),
            pltpu.VMEM((V, V), BF16),
            pltpu.VMEM((plane, rz, V), BF16),
            pltpu.VMEM((rz, V), BF16),
            pltpu.VMEM((NY - 1, rz, V), BF16),
            pltpu.VMEM((V, V), BF16),
            dma, dma, dma, dma((CHUNKS,)), dma((CHUNKS,)), dma((2,)), dma((2,)), dma, dma,
            dma((plane,)), dma((plane,)), dma((NY - 1,)), dma((NY - 1,)),
            dma((plane,)), dma((plane,)), dma((NX,)), dma((NX,)),
        ],
        compiler_params=pltpu.CompilerParams(
            collective_id=0, has_side_effects=True, vmem_limit_bytes=36 * 2**20
        ),
        cost_estimate=pl.CostEstimate(flops=flops, bytes_accessed=8 * V * A, transcendentals=0),
        name="window",
    )(
        pltpu.with_memory_space_constraint(factors.reshape(V, A), pltpu.HBM),
        table,
        pltpu.with_memory_space_constraint(jnp.transpose(pair_code, (2, 0, 1)), pltpu.HBM),
        pltpu.with_memory_space_constraint(pair_count, pltpu.HBM),
    )
    return aux.reshape(1, V, A), lag.reshape(1, V, A)


def solution(mesh):
    in_specs = (
        P(("grp", "mem"), None, None),
        P(("grp", "mem")),
        P(),
        P("grp", None, None),
        P("grp", None),
    )
    out_specs = (P(("grp", "mem"), None, None), P(("grp", "mem"), None, None))
    return jax.shard_map(
        per_device, mesh=mesh, in_specs=in_specs, out_specs=out_specs, check_vma=False
    )
```

```python
import functools

import jax
import jax.numpy as jnp
from jax import lax
from jax.experimental import pallas as pl
from jax.experimental.pallas import tpu as pltpu
from jax.sharding import PartitionSpec as P

MESH = pl.DeviceIdType.MESH
NX, NY, NZ = 4, 4, 8
CHUNKS = 16
LEAD = 1
LAST = 384
STEPS = 4
FAR_FIRST = sorted(
    range(1, NX * NZ),
    key=lambda d: (-min(d // NZ, NX - d // NZ) - min(d % NZ, NZ - d % NZ), d),
)
F32, BF16 = jnp.float32, jnp.bfloat16


def nt(a, b):
    return lax.dot_general(a, b, (((1,), (1,)), ((), ())), preferred_element_type=F32)


def tn(a, b):
    return lax.dot_general(a, b, (((0,), (0,)), ((), ())), preferred_element_type=F32)


def nn(a, b):
    return jnp.dot(a, b, preferred_element_type=F32)


def body(
    b_hbm, table, code, count,
    gamma_out, dfull,
    b_own, ball, tall, ens, vsum, acc, dens, dl_send, dl_recv, xs, pr, ys, yr,
    load_sem, pair_s, pair_r, bulk_s, bulk_r, en_s, en_r, dl_s, dl_rs,
    p_s, p_r, y_s, y_r, f_s, f_r, fw_s, fw_r, go,
):
    V, A = b_hbm.shape
    g, m = lax.axis_index("grp"), lax.axis_index("mem")
    x, ylo = lax.rem(g, NX), g // NX
    core, yhi, z = lax.rem(m, 2), lax.rem(m // 2, 2), m // 4
    y = yhi * 2 + ylo
    mate = m + 1 - 2 * core
    far = m + 2 - 4 * yhi
    early = core == yhi
    late = core != yhi
    rows_x, rows_z = V // NX, V // NX // NZ

    load = pltpu.make_async_copy(b_hbm, b_own, load_sem)
    load.start()

    def to_plane(d):
        dx, dz = d // NZ, d % NZ
        return {
            "grp": ylo * NX + lax.rem(x + dx, NX),
            "mem": lax.rem(z + dz, NZ) * 4 + yhi * 2 + 1 - yhi,
        }

    def to_plane_early(d):
        dx, dz = d // NZ, d % NZ
        return {
            "grp": ylo * NX + lax.rem(x + dx, NX),
            "mem": lax.rem(z + dz, NZ) * 4 + yhi * 2 + yhi,
        }

    def late_y(d):
        other = lax.rem(y + d, NY)
        hi, lo = other // 2, lax.rem(other, 2)
        return {"grp": lo * NX + x, "mem": z * 4 + hi * 2 + 1 - hi}

    def early_y(d):
        other = lax.rem(y + d, NY)
        hi, lo = other // 2, lax.rem(other, 2)
        return {"grp": lo * NX + x, "mem": z * 4 + hi * 3}

    to_mate = {"grp": g, "mem": mate}
    to_far = {"grp": g, "mem": far}

    barrier = pltpu.get_barrier_semaphore()

    def greet(where):
        pl.semaphore_signal(barrier, inc=1, device_id=where, device_id_type=MESH)

    def remote(src, dst, send, recv, where):
        return pltpu.make_async_remote_copy(
            src_ref=src, dst_ref=dst, send_sem=send, recv_sem=recv, device_id=where, device_id_type=MESH
        )

    greet(to_mate)
    greet(to_far)

    @pl.when(late)
    def _():
        for d in FAR_FIRST:
            greet(to_plane_early(d))
        for d in range(1, NY):
            greet(early_y(d))

    crows = V // CHUNKS

    def bulk(i):
        r = pl.ds(pl.multiple_of(i * crows, crows), crows)
        return remote(b_own.at[r], ball.at[1, r], bulk_s.at[i], bulk_r.at[i], to_far)

    def bulk_start(lo, hi):
        @pl.loop(lo, hi)
        def _(i):
            bulk(i).start()

    def bulk_wait(lo, hi):
        @pl.loop(lo, hi)
        def _(i):
            bulk(i).wait_recv()

    pair = remote(b_own, ball.at[0], pair_s, pair_r, to_mate)
    en1 = remote(table.at[8:16], ens.at[0], en_s.at[0], en_r.at[0], to_mate)
    en2 = remote(table.at[8:16], ens.at[1], en_s.at[1], en_r.at[1], to_far)

    @pl.when(late)
    def _():
        pl.semaphore_wait(barrier, 2)

    @pl.when(early)
    def _():
        pl.semaphore_wait(barrier, 2 + NX * NZ - 1 + NY - 1)

    @pl.when(early)
    def _():
        pl.semaphore_signal(go, inc=1, device_id=to_mate, device_id_type=MESH)

    en1.start()
    en2.start()
    load.wait()

    @pl.when(late)
    def _():
        bulk_start(0, CHUNKS)

    pair.start()

    def lives(who, rnd):
        total = jnp.int32(0)
        for s in range(code.shape[0]):
            hit = jnp.logical_and(code[s, 0, who] == rnd, s < count[0, who])
            total = total + jnp.where(hit, 1, 0)
        return total.astype(F32)

    c0, c1, c2 = lives(m, 0), lives(m, 1), lives(m, 2)
    d1, d2 = lives(mate, 1), lives(far, 2)

    for i in range(V // 128):
        column = jnp.broadcast_to(table[0:1, i * 128 : (i + 1) * 128], (128, 128)).T
        for j in range(V // 128):
            vsum[i * 128 : (i + 1) * 128, j * 128 : (j + 1) * 128] = column + table[0:1, j * 128 : (j + 1) * 128]

    acc[...] = jnp.zeros_like(acc)
    dens[...] = jnp.zeros_like(dens)
    own = table[8:9, 0:1]
    blocks = (b_own, ball.at[0], ball.at[1])

    def tile(r, lo, width, other):
        cols = pl.ds(pl.multiple_of(lo, 128), width)
        k = nt(b_own[...], blocks[r][cols, :])
        denominator = vsum[:, cols] - own - other
        tall[r, :, cols] = (k / denominator).astype(BF16)

    def gamma(r, lo, width, weight):
        rows = pl.ds(pl.multiple_of(lo, 128), width)

        @pl.loop(0, A // 256)
        def _(p):
            c = pl.ds(pl.multiple_of(p * 256, 256), 256)
            acc[:, c] = acc[:, c] + weight * nn(tall[r, :, rows], blocks[r][rows, c])

    def outer(r, lo, width, weight):
        cols = pl.ds(pl.multiple_of(lo, 128), width)

        @pl.loop(0, V // 256)
        def _(p):
            c = pl.ds(pl.multiple_of(p * 256, 256), 256)
            dens[:, c] = dens[:, c] + weight * nt(tall[r, :, cols], tall[r, c, cols])

    def inner(r, weight):
        @pl.loop(0, V // 256)
        def _(p):
            c = pl.ds(pl.multiple_of(p * 256, 256), 256)
            dens[:, c] = dens[:, c] + weight * tn(tall[r], tall[r, :, c])

    def whole(r, other, outer_weight, gamma_weight):
        @pl.loop(0, V // 256)
        def _(p):
            tile(r, p * 256, 256, other)

        outer(r, 0, V, outer_weight)
        gamma(r, 0, V, gamma_weight)

    whole(0, own, c0, c0 + c0)
    en1.wait_recv()
    pair.wait_recv()
    whole(1, ens[0, 0:1, 0:1], c1, c1 + d1)

    dl = remote(dl_send, dl_recv, dl_s, dl_rs, to_mate)

    @pl.when(late)
    def _():
        dl_send[...] = dens[...].astype(BF16)
        dl.start()

    en2.wait_recv()
    w2 = c2 + d2
    far_energy = ens[1, 0:1, 0:1]

    Q = CHUNKS // 4

    @pl.when(early)
    def _():
        bulk_wait(0, 2 * Q)
        tile(2, 0, 256, far_energy)
        outer(2, 0, 256, c2)
        gamma(2, 0, 256, w2)
        bulk_wait(2 * Q, 3 * Q)
        tile(2, 256, 128, far_energy)
        outer(2, 256, 128, c2)
        gamma(2, 256, 128, w2)
        dl.wait_recv()

        @pl.loop(0, V // 256)
        def _(p):
            c = pl.ds(pl.multiple_of(p * 256, 256), 256)
            dens[:, c] = dens[:, c] + dl_recv[:, c].astype(F32)

        for lo in (0, 128, 256):
            rows = slice(lo, lo + 128)
            dens[rows, 0:LAST] = dens[rows, 0:LAST] + d2 * tn(tall[2, :, rows], tall[2, :, 0:LAST])

        bulk_wait(3 * Q, CHUNKS - LEAD)
        bulk_start(0, CHUNKS)
        bulk_wait(CHUNKS - LEAD, CHUNKS)
        tile(2, LAST, 128, far_energy)

    def piece(d):
        dx, dz = d // NZ, d % NZ
        return pl.ds(
            pl.multiple_of(lax.rem(x + dx, NX) * rows_x + lax.rem(z + dz, NZ) * rows_z, rows_z), rows_z
        )

    def back(d):
        dx, dz = d // NZ, d % NZ
        return ((NX - dx) % NX) * NZ + (NZ - dz) % NZ

    def block_x(d):
        return pl.ds(pl.multiple_of(lax.rem(x + d, NX) * rows_x, rows_x), rows_x)

    def part_copy(d):
        return remote(xs.at[piece(d)], pr.at[d], p_s.at[d], p_r.at[d], to_plane(d))

    def y_copy(d):
        return remote(ys, yr.at[d - 1], y_s.at[d - 1], y_r.at[d - 1], late_y(d))

    def full_copy(d):
        r = piece(0)
        return remote(dfull.at[r], dfull.at[r], f_s.at[d - 1], f_r.at[d - 1], to_plane(d))

    def full_arrival(d):
        r = piece(back(d))
        return remote(dfull.at[r], dfull.at[r], f_s.at[d - 1], f_r.at[d - 1], to_plane(d))

    def fw_copy(d):
        r = block_x((NX - d) % NX)
        return remote(dfull.at[r], dfull.at[r], fw_s.at[d], fw_r.at[d], to_mate)

    x_order = (0, 1, 3, 2)

    @pl.when(early)
    def _():
        new = tall[2, :, LAST:V]
        dens[0:LAST, LAST:V] = dens[0:LAST, LAST:V] + d2 * tn(tall[2, :, 0:LAST], new)
        dens[LAST:V, :] = dens[LAST:V, :] + d2 * tn(new, tall[2])

        @pl.loop(0, V // 256)
        def _(p):
            c = pl.ds(pl.multiple_of(p * 256, 256), 256)
            xs[:, c] = (dens[:, c] + c2 * nt(new, tall[2, c, LAST:V])).astype(BF16)

        for d in FAR_FIRST + [0]:
            part_copy(d).start()
        gamma(2, LAST, 128, w2)
        gamma_out[...] = acc[...].astype(BF16)
        for dx in x_order:
            fw_copy(dx).wait_recv()

    @pl.when(late)
    def _():
        bulk_wait(0, Q)
        tile(2, 0, 128, far_energy)
        pl.semaphore_wait(go, 1)
        total = jnp.zeros((rows_z, V), F32)
        for d in [0] + FAR_FIRST[::-1]:
            part_copy(d).wait_recv()
            total = total + pr[d].astype(F32)
        ys[...] = total.astype(BF16)
        for d in (2, 1, 3):
            y_copy(d).start()
        for d in (1, 3, 2):
            y_copy(d).wait_recv()
            total = total + yr[d - 1].astype(F32)
        dfull[piece(0), :] = (total * (1.0 / (8.0 * 2 * NX * NY * NZ))).astype(BF16)
        for d in FAR_FIRST:
            full_copy(d).start()
        bulk_wait(Q, 2 * Q)
        tile(2, 128, 128, far_energy)
        bulk_wait(2 * Q, 3 * Q)
        tile(2, 256, 128, far_energy)
        gamma(2, 0, LAST, w2)
        bulk_wait(3 * Q, CHUNKS)
        tile(2, LAST, 128, far_energy)
        gamma(2, LAST, 128, w2)
        gamma_out[...] = acc[...].astype(BF16)
        for dx in x_order:
            for dz in (0, 1, 7, 2, 6, 3, 5, 4):
                if dx or dz:
                    full_arrival(dx * NZ + dz).wait_recv()
            fw_copy(dx).start()

    en1.wait_send()
    en2.wait_send()
    pair.wait_send()

    @pl.loop(0, CHUNKS)
    def _(i):
        bulk(i).wait_send()

    @pl.when(late)
    def _():
        dl.wait_send()
        for d in range(1, NY):
            y_copy(d).wait_send()
        for d in range(1, NX * NZ):
            full_copy(d).wait_send()
        for d in range(NX):
            fw_copy(d).wait_send()

    @pl.when(early)
    def _():
        for d in range(NX * NZ):
            part_copy(d).wait_send()


def finish(b, d, g, aux, lag, stage, aux_sem, lag_sem):
    out = pltpu.make_async_copy(g, aux, aux_sem)
    out.start()
    A = b.shape[1]
    width = A // lag_sem.shape[0]

    def copy(p):
        c = pl.ds(pl.multiple_of(p * width, 128), width)
        return pltpu.make_async_copy(stage.at[:, c], lag.at[:, c], lag_sem.at[p])

    @pl.loop(0, A // width)
    def _(p):
        c = pl.ds(pl.multiple_of(p * width, 128), width)
        stage[:, c] = nn(d[...], b[:, c]).astype(BF16)
        copy(p).start()

    @pl.loop(0, A // width)
    def _(p):
        copy(p).wait()

    out.wait()


def per_device(factors, occ_energy, vir_energy, pair_code, pair_count):
    _, V, A = factors.shape
    table = jnp.concatenate(
        [
            jnp.broadcast_to(vir_energy.astype(F32)[None, :], (8, V)),
            jnp.broadcast_to(occ_energy.astype(F32)[:, None], (8, V)),
        ]
    )
    dma = pltpu.SemaphoreType.DMA
    vmem, smem = pl.BlockSpec(memory_space=pltpu.VMEM), pl.BlockSpec(memory_space=pltpu.SMEM)
    rz, plane = V // NX // NZ, NX * NZ - 1
    flops = 2 * V * V * A * 7
    gamma, density = pl.pallas_call(
        body,
        out_shape=[jax.ShapeDtypeStruct((V, A), BF16), jax.ShapeDtypeStruct((V, V), BF16)],
        in_specs=[pl.BlockSpec(memory_space=pltpu.HBM), vmem, smem, smem],
        out_specs=[vmem, vmem],
        scratch_shapes=[
            pltpu.VMEM((V, A), BF16),
            pltpu.VMEM((2, V, A), BF16),
            pltpu.VMEM((3, V, V), BF16),
            pltpu.VMEM((2, 8, V), F32),
            pltpu.VMEM((V, V), F32),
            pltpu.VMEM((V, A), F32),
            pltpu.VMEM((V, V), F32),
            pltpu.VMEM((V, V), BF16),
            pltpu.VMEM((V, V), BF16),
            pltpu.VMEM((V, V), BF16),
            pltpu.VMEM((NX * NZ, rz, V), BF16),
            pltpu.VMEM((rz, V), BF16),
            pltpu.VMEM((NY - 1, rz, V), BF16),
            dma, dma, dma, dma((CHUNKS,)), dma((CHUNKS,)), dma((2,)), dma((2,)), dma, dma,
            dma((NX * NZ,)), dma((NX * NZ,)), dma((NY - 1,)), dma((NY - 1,)),
            dma((plane,)), dma((plane,)), dma((NX,)), dma((NX,)),
            pltpu.SemaphoreType.REGULAR,
        ],
        compiler_params=pltpu.CompilerParams(
            collective_id=0, has_side_effects=True, vmem_limit_bytes=36 * 2**20
        ),
        cost_estimate=pl.CostEstimate(flops=flops, bytes_accessed=8 * V * A, transcendentals=0),
        name="window",
    )(
        pltpu.with_memory_space_constraint(factors.reshape(V, A), pltpu.HBM),
        table,
        pltpu.with_memory_space_constraint(jnp.transpose(pair_code, (2, 0, 1)), pltpu.HBM),
        pltpu.with_memory_space_constraint(pair_count, pltpu.HBM),
    )
    anywhere = pl.BlockSpec(memory_space=pltpu.HBM)
    aux, lag = pl.pallas_call(
        finish,
        out_shape=[jax.ShapeDtypeStruct((V, A), BF16)] * 2,
        in_specs=[vmem, vmem, vmem],
        out_specs=[anywhere, anywhere],
        scratch_shapes=[pltpu.VMEM((V, A), BF16), dma, dma((STEPS,))],
        compiler_params=pltpu.CompilerParams(vmem_limit_bytes=16 * 2**20),
        cost_estimate=pl.CostEstimate(flops=2 * V * V * A, bytes_accessed=8 * V * A, transcendentals=0),
        name="finish",
    )(factors.reshape(V, A), density, gamma)
    return aux.reshape(1, V, A), lag.reshape(1, V, A)


def solution(mesh):
    in_specs = (
        P(("grp", "mem"), None, None),
        P(("grp", "mem")),
        P(),
        P("grp", None, None),
        P("grp", None),
    )
    out_specs = (P(("grp", "mem"), None, None), P(("grp", "mem"), None, None))
    return jax.shard_map(
        per_device, mesh=mesh, in_specs=in_specs, out_specs=out_specs, check_vma=False
    )
```

```python
import functools

import jax
import jax.numpy as jnp
from jax import lax
from jax.experimental import pallas as pl
from jax.experimental.pallas import tpu as pltpu
from jax.sharding import PartitionSpec as P

MESH = pl.DeviceIdType.MESH
NX, NY, NZ = 4, 4, 8
CHUNKS = 16
LEAD = 1
FIRST = 4
LAST = 384
STEPS = 4
FAR_FIRST = sorted(
    range(1, NX * NZ),
    key=lambda d: (-min(d // NZ, NX - d // NZ) - min(d % NZ, NZ - d % NZ), d),
)
F32, BF16 = jnp.float32, jnp.bfloat16


def nt(a, b):
    return lax.dot_general(a, b, (((1,), (1,)), ((), ())), preferred_element_type=F32)


def tn(a, b):
    return lax.dot_general(a, b, (((0,), (0,)), ((), ())), preferred_element_type=F32)


def nn(a, b):
    return jnp.dot(a, b, preferred_element_type=F32)


def body(
    b_hbm, table, code, count,
    gamma_out, dfull,
    b_own, ball, tall, ens, vsum, acc, dens, dl_send, dl_recv, xs, pr, ys, yr,
    load_sem, pair_s, pair_r, bulk_s, bulk_r, en_s, en_r, dl_s, dl_rs,
    p_s, p_r, y_s, y_r, f_s, f_r, fw_s, fw_r, go,
):
    V, A = b_hbm.shape
    g, m = lax.axis_index("grp"), lax.axis_index("mem")
    x, ylo = lax.rem(g, NX), g // NX
    core, yhi, z = lax.rem(m, 2), lax.rem(m // 2, 2), m // 4
    y = yhi * 2 + ylo
    mate = m + 1 - 2 * core
    far = m + 2 - 4 * yhi
    early = core == yhi
    late = core != yhi
    rows_x, rows_z = V // NX, V // NX // NZ

    load = pltpu.make_async_copy(b_hbm, b_own, load_sem)
    load.start()

    def to_plane(d):
        dx, dz = d // NZ, d % NZ
        return {
            "grp": ylo * NX + lax.rem(x + dx, NX),
            "mem": lax.rem(z + dz, NZ) * 4 + yhi * 2 + 1 - yhi,
        }

    def to_plane_early(d):
        dx, dz = d // NZ, d % NZ
        return {
            "grp": ylo * NX + lax.rem(x + dx, NX),
            "mem": lax.rem(z + dz, NZ) * 4 + yhi * 2 + yhi,
        }

    def late_y(d):
        other = lax.rem(y + d, NY)
        hi, lo = other // 2, lax.rem(other, 2)
        return {"grp": lo * NX + x, "mem": z * 4 + hi * 2 + 1 - hi}

    def early_y(d):
        other = lax.rem(y + d, NY)
        hi, lo = other // 2, lax.rem(other, 2)
        return {"grp": lo * NX + x, "mem": z * 4 + hi * 3}

    to_mate = {"grp": g, "mem": mate}
    to_far = {"grp": g, "mem": far}

    barrier = pltpu.get_barrier_semaphore()

    def greet(where):
        pl.semaphore_signal(barrier, inc=1, device_id=where, device_id_type=MESH)

    def remote(src, dst, send, recv, where):
        return pltpu.make_async_remote_copy(
            src_ref=src, dst_ref=dst, send_sem=send, recv_sem=recv, device_id=where, device_id_type=MESH
        )

    greet(to_mate)
    greet(to_far)

    @pl.when(late)
    def _():
        for d in FAR_FIRST:
            greet(to_plane_early(d))
        for d in range(1, NY):
            greet(early_y(d))

    crows = V // CHUNKS

    def bulk(i):
        r = pl.ds(pl.multiple_of(i * crows, crows), crows)
        return remote(b_own.at[r], ball.at[1, r], bulk_s.at[i], bulk_r.at[i], to_far)

    def bulk_start(lo, hi):
        @pl.loop(lo, hi)
        def _(i):
            bulk(i).start()

    def bulk_wait(lo, hi):
        @pl.loop(lo, hi)
        def _(i):
            bulk(i).wait_recv()

    pair = remote(b_own, ball.at[0], pair_s, pair_r, to_mate)
    en1 = remote(table.at[8:16], ens.at[0], en_s.at[0], en_r.at[0], to_mate)
    en2 = remote(table.at[8:16], ens.at[1], en_s.at[1], en_r.at[1], to_far)

    @pl.when(late)
    def _():
        pl.semaphore_wait(barrier, 2)

    @pl.when(early)
    def _():
        pl.semaphore_wait(barrier, 2 + NX * NZ - 1 + NY - 1)

    @pl.when(early)
    def _():
        pl.semaphore_signal(go, inc=1, device_id=to_mate, device_id_type=MESH)

    en1.start()
    en2.start()
    load.wait()

    @pl.when(late)
    def _():
        bulk_start(0, CHUNKS)

    pair.start()

    def lives(who, rnd):
        total = jnp.int32(0)
        for s in range(code.shape[0]):
            hit = jnp.logical_and(code[s, 0, who] == rnd, s < count[0, who])
            total = total + jnp.where(hit, 1, 0)
        return total.astype(F32)

    c0, c1, c2 = lives(m, 0), lives(m, 1), lives(m, 2)
    d1, d2 = lives(mate, 1), lives(far, 2)

    for i in range(V // 128):
        column = jnp.broadcast_to(table[0:1, i * 128 : (i + 1) * 128], (128, 128)).T
        for j in range(V // 128):
            vsum[i * 128 : (i + 1) * 128, j * 128 : (j + 1) * 128] = column + table[0:1, j * 128 : (j + 1) * 128]

    acc[...] = jnp.zeros_like(acc)
    dens[...] = jnp.zeros_like(dens)
    own = table[8:9, 0:1]
    blocks = (b_own, ball.at[0], ball.at[1])

    def tile(r, lo, width, other):
        cols = pl.ds(pl.multiple_of(lo, 128), width)
        k = nt(b_own[...], blocks[r][cols, :])
        denominator = vsum[:, cols] - own - other
        tall[r, :, cols] = (k / denominator).astype(BF16)

    def gamma(r, lo, width, weight):
        rows = pl.ds(pl.multiple_of(lo, 128), width)

        @pl.loop(0, A // 256)
        def _(p):
            c = pl.ds(pl.multiple_of(p * 256, 256), 256)
            acc[:, c] = acc[:, c] + weight * nn(tall[r, :, rows], blocks[r][rows, c])

    def gamma_last(lo, width, weight):
        rows = pl.ds(pl.multiple_of(lo, 128), width)

        @pl.loop(0, A // 256)
        def _(p):
            c = pl.ds(pl.multiple_of(p * 256, 256), 256)
            gamma_out[:, c] = (acc[:, c] + weight * nn(tall[2, :, rows], ball[1, rows, c])).astype(BF16)

    def outer(r, lo, width, weight):
        cols = pl.ds(pl.multiple_of(lo, 128), width)

        @pl.loop(0, V // 256)
        def _(p):
            c = pl.ds(pl.multiple_of(p * 256, 256), 256)
            dens[:, c] = dens[:, c] + weight * nt(tall[r, :, cols], tall[r, c, cols])

    def inner(r, weight):
        @pl.loop(0, V // 256)
        def _(p):
            c = pl.ds(pl.multiple_of(p * 256, 256), 256)
            dens[:, c] = dens[:, c] + weight * tn(tall[r], tall[r, :, c])

    def whole(r, other, outer_weight, gamma_weight):
        @pl.loop(0, V // 256)
        def _(p):
            tile(r, p * 256, 256, other)

        outer(r, 0, V, outer_weight)
        gamma(r, 0, V, gamma_weight)

    whole(0, own, c0, c0 + c0)
    en1.wait_recv()
    pair.wait_recv()
    whole(1, ens[0, 0:1, 0:1], c1, c1 + d1)

    dl = remote(dl_send, dl_recv, dl_s, dl_rs, to_mate)

    @pl.when(late)
    def _():
        dl_send[...] = dens[...].astype(BF16)
        dl.start()

    en2.wait_recv()
    w2 = c2 + d2
    far_energy = ens[1, 0:1, 0:1]

    Q = CHUNKS // 4

    @pl.when(early)
    def _():
        bulk_wait(0, 2 * Q)
        tile(2, 0, 256, far_energy)
        outer(2, 0, 256, c2)
        gamma(2, 0, 256, w2)
        bulk_wait(2 * Q, 3 * Q)
        tile(2, 256, 128, far_energy)
        outer(2, 256, 128, c2)
        gamma(2, 256, 128, w2)
        dl.wait_recv()

        @pl.loop(0, V // 256)
        def _(p):
            c = pl.ds(pl.multiple_of(p * 256, 256), 256)
            dens[:, c] = dens[:, c] + dl_recv[:, c].astype(F32)

        for lo in (0, 128, 256):
            rows = slice(lo, lo + 128)
            dens[rows, 0:LAST] = dens[rows, 0:LAST] + d2 * tn(tall[2, :, rows], tall[2, :, 0:LAST])

        bulk_wait(3 * Q, CHUNKS - LEAD)
        bulk_start(0, FIRST)
        bulk_wait(CHUNKS - LEAD, CHUNKS)
        tile(2, LAST, 128, far_energy)

    def piece(d):
        dx, dz = d // NZ, d % NZ
        return pl.ds(
            pl.multiple_of(lax.rem(x + dx, NX) * rows_x + lax.rem(z + dz, NZ) * rows_z, rows_z), rows_z
        )

    def back(d):
        dx, dz = d // NZ, d % NZ
        return ((NX - dx) % NX) * NZ + (NZ - dz) % NZ

    def block_x(d):
        return pl.ds(pl.multiple_of(lax.rem(x + d, NX) * rows_x, rows_x), rows_x)

    def part_copy(d):
        return remote(xs.at[piece(d)], pr.at[d], p_s.at[d], p_r.at[d], to_plane(d))

    def y_copy(d):
        return remote(ys, yr.at[d - 1], y_s.at[d - 1], y_r.at[d - 1], late_y(d))

    def full_copy(d):
        r = piece(0)
        return remote(dfull.at[r], dfull.at[r], f_s.at[d - 1], f_r.at[d - 1], to_plane(d))

    def full_arrival(d):
        r = piece(back(d))
        return remote(dfull.at[r], dfull.at[r], f_s.at[d - 1], f_r.at[d - 1], to_plane(d))

    def fw_copy(d):
        r = block_x((NX - d) % NX)
        return remote(dfull.at[r], dfull.at[r], fw_s.at[d], fw_r.at[d], to_mate)

    x_order = (0, 1, 3, 2)

    @pl.when(early)
    def _():
        new = tall[2, :, LAST:V]
        dens[0:LAST, LAST:V] = dens[0:LAST, LAST:V] + d2 * tn(tall[2, :, 0:LAST], new)
        dens[LAST:V, :] = dens[LAST:V, :] + d2 * tn(new, tall[2])

        for j in range(NX):
            cols = slice(j * rows_x, (j + 1) * rows_x)
            term = dens[:, cols] + c2 * nt(new, tall[2, cols, LAST:V])
            for k in range(NX - 1):
                i = (j - k) % NX
                xs[i * rows_x : (i + 1) * rows_x, k * rows_x : (k + 1) * rows_x] = term[
                    i * rows_x : (i + 1) * rows_x
                ].astype(BF16)

        for d in FAR_FIRST + [0]:
            part_copy(d).start()
        bulk_start(FIRST, CHUNKS)
        gamma_last(LAST, 128, w2)
        for dx in x_order:
            fw_copy(dx).wait_recv()

    @pl.when(late)
    def _():
        bulk_wait(0, Q)
        tile(2, 0, 128, far_energy)
        pl.semaphore_wait(go, 1)
        total = jnp.zeros((rows_z, xs.shape[1]), F32)
        for d in [0] + FAR_FIRST[::-1]:
            part_copy(d).wait_recv()
            total = total + pr[d].astype(F32)
        ys[...] = total.astype(BF16)
        for d in (2, 1, 3):
            y_copy(d).start()
        for d in (1, 3, 2):
            y_copy(d).wait_recv()
            total = total + yr[d - 1].astype(F32)
        dfull[piece(0), :] = (total * (1.0 / (8.0 * 2 * NX * NY * NZ))).astype(BF16)
        for d in FAR_FIRST:
            full_copy(d).start()
        bulk_wait(Q, 2 * Q)
        tile(2, 128, 128, far_energy)
        bulk_wait(2 * Q, 3 * Q)
        tile(2, 256, 128, far_energy)
        gamma(2, 0, LAST, w2)
        bulk_wait(3 * Q, CHUNKS)
        tile(2, LAST, 128, far_energy)
        gamma_last(LAST, 128, w2)
        for dx in x_order:
            for dz in (0, 1, 7, 2, 6, 3, 5, 4):
                if dx or dz:
                    full_arrival(dx * NZ + dz).wait_recv()
            fw_copy(dx).start()

    en1.wait_send()
    en2.wait_send()
    pair.wait_send()

    @pl.loop(0, CHUNKS)
    def _(i):
        bulk(i).wait_send()

    @pl.when(late)
    def _():
        dl.wait_send()
        for d in range(1, NY):
            y_copy(d).wait_send()
        for d in range(1, NX * NZ):
            full_copy(d).wait_send()
        for d in range(NX):
            fw_copy(d).wait_send()

    @pl.when(early)
    def _():
        for d in range(NX * NZ):
            part_copy(d).wait_send()


def finish(b, d, g, aux, lag, full, stage, aux_sem, lag_sem):
    out = pltpu.make_async_copy(g, aux, aux_sem)
    out.start()
    A = b.shape[1]
    width = A // lag_sem.shape[0]

    def copy(p):
        c = pl.ds(pl.multiple_of(p * width, 128), width)
        return pltpu.make_async_copy(stage.at[:, c], lag.at[:, c], lag_sem.at[p])

    n = d.shape[0] // NX
    for i in range(NX):
        rows = slice(i * n, (i + 1) * n)
        for k in range(NX - 1):
            j = (i + k) % NX
            full[rows, j * n : (j + 1) * n] = d[rows, k * n : (k + 1) * n]
        j = (i + NX - 1) % NX
        full[rows, j * n : (j + 1) * n] = d[j * n : (j + 1) * n, n : 2 * n].astype(F32).T.astype(BF16)

    @pl.loop(0, A // width)
    def _(p):
        c = pl.ds(pl.multiple_of(p * width, 128), width)
        stage[:, c] = nn(full[...], b[:, c]).astype(BF16)
        copy(p).start()

    @pl.loop(0, A // width)
    def _(p):
        copy(p).wait()

    out.wait()


def per_device(factors, occ_energy, vir_energy, pair_code, pair_count):
    _, V, A = factors.shape
    table = jnp.concatenate(
        [
            jnp.broadcast_to(vir_energy.astype(F32)[None, :], (8, V)),
            jnp.broadcast_to(occ_energy.astype(F32)[:, None], (8, V)),
        ]
    )
    dma = pltpu.SemaphoreType.DMA
    vmem, smem = pl.BlockSpec(memory_space=pltpu.VMEM), pl.BlockSpec(memory_space=pltpu.SMEM)
    W = V - V // NX
    rz, plane = V // NX // NZ, NX * NZ - 1
    flops = 2 * V * V * A * 7
    gamma, density = pl.pallas_call(
        body,
        out_shape=[jax.ShapeDtypeStruct((V, A), BF16), jax.ShapeDtypeStruct((V, W), BF16)],
        in_specs=[pl.BlockSpec(memory_space=pltpu.HBM), vmem, smem, smem],
        out_specs=[vmem, vmem],
        scratch_shapes=[
            pltpu.VMEM((V, A), BF16),
            pltpu.VMEM((2, V, A), BF16),
            pltpu.VMEM((3, V, V), BF16),
            pltpu.VMEM((2, 8, V), F32),
            pltpu.VMEM((V, V), F32),
            pltpu.VMEM((V, A), F32),
            pltpu.VMEM((V, V), F32),
            pltpu.VMEM((V, V), BF16),
            pltpu.VMEM((V, V), BF16),
            pltpu.VMEM((V, W), BF16),
            pltpu.VMEM((NX * NZ, rz, W), BF16),
            pltpu.VMEM((rz, W), BF16),
            pltpu.VMEM((NY - 1, rz, W), BF16),
            dma, dma, dma, dma((CHUNKS,)), dma((CHUNKS,)), dma((2,)), dma((2,)), dma, dma,
            dma((NX * NZ,)), dma((NX * NZ,)), dma((NY - 1,)), dma((NY - 1,)),
            dma((plane,)), dma((plane,)), dma((NX,)), dma((NX,)),
            pltpu.SemaphoreType.REGULAR,
        ],
        compiler_params=pltpu.CompilerParams(
            collective_id=0, has_side_effects=True, vmem_limit_bytes=36 * 2**20
        ),
        cost_estimate=pl.CostEstimate(flops=flops, bytes_accessed=8 * V * A, transcendentals=0),
        name="window",
    )(
        pltpu.with_memory_space_constraint(factors.reshape(V, A), pltpu.HBM),
        table,
        pltpu.with_memory_space_constraint(jnp.transpose(pair_code, (2, 0, 1)), pltpu.HBM),
        pltpu.with_memory_space_constraint(pair_count, pltpu.HBM),
    )
    anywhere = pl.BlockSpec(memory_space=pltpu.HBM)
    aux, lag = pl.pallas_call(
        finish,
        out_shape=[jax.ShapeDtypeStruct((V, A), BF16)] * 2,
        in_specs=[vmem, vmem, vmem],
        out_specs=[anywhere, anywhere],
        scratch_shapes=[pltpu.VMEM((V, V), BF16), pltpu.VMEM((V, A), BF16), dma, dma((STEPS,))],
        compiler_params=pltpu.CompilerParams(vmem_limit_bytes=16 * 2**20),
        cost_estimate=pl.CostEstimate(flops=2 * V * V * A, bytes_accessed=8 * V * A, transcendentals=0),
        name="finish",
    )(factors.reshape(V, A), density, gamma)
    return aux.reshape(1, V, A), lag.reshape(1, V, A)


def solution(mesh):
    in_specs = (
        P(("grp", "mem"), None, None),
        P(("grp", "mem")),
        P(),
        P("grp", None, None),
        P("grp", None),
    )
    out_specs = (P(("grp", "mem"), None, None), P(("grp", "mem"), None, None))
    return jax.shard_map(
        per_device, mesh=mesh, in_specs=in_specs, out_specs=out_specs, check_vma=False
    )
```

```python
import functools

import jax
import jax.numpy as jnp
from jax import lax
from jax.experimental import pallas as pl
from jax.experimental.pallas import tpu as pltpu
from jax.sharding import PartitionSpec as P

MESH = pl.DeviceIdType.MESH
NX, NY, NZ = 4, 4, 8
CHUNKS = 16
LEAD = 2
FIRST = 5
LAST = 384
STEPS = 4
FAR_FIRST = sorted(
    range(1, NX * NZ),
    key=lambda d: (-min(d // NZ, NX - d // NZ) - min(d % NZ, NZ - d % NZ), d),
)
F32, BF16 = jnp.float32, jnp.bfloat16


def nt(a, b):
    return lax.dot_general(a, b, (((1,), (1,)), ((), ())), preferred_element_type=F32)


def tn(a, b):
    return lax.dot_general(a, b, (((0,), (0,)), ((), ())), preferred_element_type=F32)


def nn(a, b):
    return jnp.dot(a, b, preferred_element_type=F32)


def body(
    b_hbm, table, code, count,
    gamma_out, dfull,
    b_own, ball, tall, ens, vsum, acc, dens, dl_send, dl_recv, xs, pr, ys, yr,
    load_sem, pair_s, pair_r, bulk_s, bulk_r, en_s, en_r, dl_s, dl_rs,
    p_s, p_r, y_s, y_r, f_s, f_r, fw_s, fw_r, go,
):
    V, A = b_hbm.shape
    g, m = lax.axis_index("grp"), lax.axis_index("mem")
    x, ylo = lax.rem(g, NX), g // NX
    core, yhi, z = lax.rem(m, 2), lax.rem(m // 2, 2), m // 4
    y = yhi * 2 + ylo
    mate = m + 1 - 2 * core
    far = m + 2 - 4 * yhi
    early = core == yhi
    late = core != yhi
    rows_x, rows_z = V // NX, V // NX // NZ

    load = pltpu.make_async_copy(b_hbm, b_own, load_sem)
    load.start()

    def to_plane(d):
        dx, dz = d // NZ, d % NZ
        return {
            "grp": ylo * NX + lax.rem(x + dx, NX),
            "mem": lax.rem(z + dz, NZ) * 4 + yhi * 2 + 1 - yhi,
        }

    def to_plane_early(d):
        dx, dz = d // NZ, d % NZ
        return {
            "grp": ylo * NX + lax.rem(x + dx, NX),
            "mem": lax.rem(z + dz, NZ) * 4 + yhi * 2 + yhi,
        }

    def late_y(d):
        other = lax.rem(y + d, NY)
        hi, lo = other // 2, lax.rem(other, 2)
        return {"grp": lo * NX + x, "mem": z * 4 + hi * 2 + 1 - hi}

    def early_y(d):
        other = lax.rem(y + d, NY)
        hi, lo = other // 2, lax.rem(other, 2)
        return {"grp": lo * NX + x, "mem": z * 4 + hi * 3}

    to_mate = {"grp": g, "mem": mate}
    to_far = {"grp": g, "mem": far}

    barrier = pltpu.get_barrier_semaphore()

    def greet(where):
        pl.semaphore_signal(barrier, inc=1, device_id=where, device_id_type=MESH)

    def remote(src, dst, send, recv, where):
        return pltpu.make_async_remote_copy(
            src_ref=src, dst_ref=dst, send_sem=send, recv_sem=recv, device_id=where, device_id_type=MESH
        )

    greet(to_mate)
    greet(to_far)

    @pl.when(late)
    def _():
        for d in FAR_FIRST:
            greet(to_plane_early(d))
        for d in range(1, NY):
            greet(early_y(d))

    crows = V // CHUNKS

    def bulk(i):
        r = pl.ds(pl.multiple_of(i * crows, crows), crows)
        return remote(b_own.at[r], ball.at[1, r], bulk_s.at[i], bulk_r.at[i], to_far)

    def bulk_start(lo, hi):
        @pl.loop(lo, hi)
        def _(i):
            bulk(i).start()

    def bulk_wait(lo, hi):
        @pl.loop(lo, hi)
        def _(i):
            bulk(i).wait_recv()

    pair = remote(b_own, ball.at[0], pair_s, pair_r, to_mate)
    en1 = remote(table.at[8:16], ens.at[0], en_s.at[0], en_r.at[0], to_mate)
    en2 = remote(table.at[8:16], ens.at[1], en_s.at[1], en_r.at[1], to_far)

    @pl.when(late)
    def _():
        pl.semaphore_wait(barrier, 2)

    @pl.when(early)
    def _():
        pl.semaphore_wait(barrier, 2 + NX * NZ - 1 + NY - 1)

    @pl.when(early)
    def _():
        pl.semaphore_signal(go, inc=1, device_id=to_mate, device_id_type=MESH)

    en1.start()
    en2.start()
    load.wait()

    @pl.when(late)
    def _():
        bulk_start(0, CHUNKS)

    pair.start()

    def lives(who, rnd):
        total = jnp.int32(0)
        for s in range(code.shape[0]):
            hit = jnp.logical_and(code[s, 0, who] == rnd, s < count[0, who])
            total = total + jnp.where(hit, 1, 0)
        return total.astype(F32)

    c0, c1, c2 = lives(m, 0), lives(m, 1), lives(m, 2)
    d1, d2 = lives(mate, 1), lives(far, 2)

    for i in range(V // 128):
        column = jnp.broadcast_to(table[0:1, i * 128 : (i + 1) * 128], (128, 128)).T
        for j in range(V // 128):
            vsum[i * 128 : (i + 1) * 128, j * 128 : (j + 1) * 128] = column + table[0:1, j * 128 : (j + 1) * 128]

    acc[...] = jnp.zeros_like(acc)
    dens[...] = jnp.zeros_like(dens)
    own = table[8:9, 0:1]
    blocks = (b_own, ball.at[0], ball.at[1])

    def tile(r, lo, width, other):
        cols = pl.ds(pl.multiple_of(lo, 128), width)
        k = nt(b_own[...], blocks[r][cols, :])
        denominator = vsum[:, cols] - own - other
        tall[r, :, cols] = (k / denominator).astype(BF16)

    def gamma(r, lo, width, weight):
        rows = pl.ds(pl.multiple_of(lo, 128), width)

        @pl.loop(0, A // 256)
        def _(p):
            c = pl.ds(pl.multiple_of(p * 256, 256), 256)
            acc[:, c] = acc[:, c] + weight * nn(tall[r, :, rows], blocks[r][rows, c])

    def gamma_last(lo, width, weight):
        rows = pl.ds(pl.multiple_of(lo, 128), width)

        @pl.loop(0, A // 256)
        def _(p):
            c = pl.ds(pl.multiple_of(p * 256, 256), 256)
            gamma_out[:, c] = (acc[:, c] + weight * nn(tall[2, :, rows], ball[1, rows, c])).astype(BF16)

    def outer(r, lo, width, weight):
        cols = pl.ds(pl.multiple_of(lo, 128), width)

        @pl.loop(0, V // 256)
        def _(p):
            c = pl.ds(pl.multiple_of(p * 256, 256), 256)
            dens[:, c] = dens[:, c] + weight * nt(tall[r, :, cols], tall[r, c, cols])

    def inner(r, weight):
        @pl.loop(0, V // 256)
        def _(p):
            c = pl.ds(pl.multiple_of(p * 256, 256), 256)
            dens[:, c] = dens[:, c] + weight * tn(tall[r], tall[r, :, c])

    def whole(r, other, outer_weight, gamma_weight):
        @pl.loop(0, V // 256)
        def _(p):
            tile(r, p * 256, 256, other)

        outer(r, 0, V, outer_weight)
        gamma(r, 0, V, gamma_weight)

    whole(0, own, c0, c0 + c0)
    en1.wait_recv()
    pair.wait_recv()
    whole(1, ens[0, 0:1, 0:1], c1, c1 + d1)

    dl = remote(dl_send, dl_recv, dl_s, dl_rs, to_mate)

    @pl.when(late)
    def _():
        dl_send[...] = dens[...].astype(BF16)
        dl.start()

    en2.wait_recv()
    w2 = c2 + d2
    far_energy = ens[1, 0:1, 0:1]

    Q = CHUNKS // 4

    @pl.when(early)
    def _():
        bulk_wait(0, 2 * Q)
        tile(2, 0, 256, far_energy)
        outer(2, 0, 256, c2)
        gamma(2, 0, 256, w2)
        bulk_wait(2 * Q, 3 * Q)
        tile(2, 256, 128, far_energy)
        outer(2, 256, 128, c2)
        gamma(2, 256, 128, w2)
        dl.wait_recv()

        @pl.loop(0, V // 256)
        def _(p):
            c = pl.ds(pl.multiple_of(p * 256, 256), 256)
            dens[:, c] = dens[:, c] + dl_recv[:, c].astype(F32)

        for lo in (0, 128, 256):
            rows = slice(lo, lo + 128)
            dens[rows, 0:LAST] = dens[rows, 0:LAST] + d2 * tn(tall[2, :, rows], tall[2, :, 0:LAST])

        bulk_wait(3 * Q, CHUNKS - LEAD)
        bulk_start(0, FIRST)
        bulk_wait(CHUNKS - LEAD, CHUNKS)
        tile(2, LAST, 128, far_energy)

    def piece(d):
        dx, dz = d // NZ, d % NZ
        return pl.ds(
            pl.multiple_of(lax.rem(x + dx, NX) * rows_x + lax.rem(z + dz, NZ) * rows_z, rows_z), rows_z
        )

    def back(d):
        dx, dz = d // NZ, d % NZ
        return ((NX - dx) % NX) * NZ + (NZ - dz) % NZ

    def block_x(d):
        return pl.ds(pl.multiple_of(lax.rem(x + d, NX) * rows_x, rows_x), rows_x)

    def part_copy(d):
        return remote(xs.at[piece(d)], pr.at[d], p_s.at[d], p_r.at[d], to_plane(d))

    def y_copy(d):
        return remote(ys, yr.at[d - 1], y_s.at[d - 1], y_r.at[d - 1], late_y(d))

    def full_copy(d):
        r = piece(0)
        return remote(dfull.at[r], dfull.at[r], f_s.at[d - 1], f_r.at[d - 1], to_plane(d))

    def full_arrival(d):
        r = piece(back(d))
        return remote(dfull.at[r], dfull.at[r], f_s.at[d - 1], f_r.at[d - 1], to_plane(d))

    def fw_copy(d):
        r = block_x((NX - d) % NX)
        return remote(dfull.at[r], dfull.at[r], fw_s.at[d], fw_r.at[d], to_mate)

    x_order = (0, 1, 3, 2)

    @pl.when(early)
    def _():
        new = tall[2, :, LAST:V]
        dens[0:LAST, LAST:V] = dens[0:LAST, LAST:V] + d2 * tn(tall[2, :, 0:LAST], new)
        dens[LAST:V, :] = dens[LAST:V, :] + d2 * tn(new, tall[2])

        for j in range(NX):
            cols = slice(j * rows_x, (j + 1) * rows_x)
            term = dens[:, cols] + c2 * nt(new, tall[2, cols, LAST:V])
            for k in range(NX - 1):
                i = (j - k) % NX
                xs[i * rows_x : (i + 1) * rows_x, k * rows_x : (k + 1) * rows_x] = term[
                    i * rows_x : (i + 1) * rows_x
                ].astype(BF16)

        for d in FAR_FIRST + [0]:
            part_copy(d).start()
        bulk_start(FIRST, CHUNKS)
        gamma_last(LAST, 128, w2)
        for dx in x_order:
            fw_copy(dx).wait_recv()

    @pl.when(late)
    def _():
        bulk_wait(0, Q)
        tile(2, 0, 128, far_energy)
        pl.semaphore_wait(go, 1)
        total = jnp.zeros((rows_z, xs.shape[1]), F32)
        for d in [0] + FAR_FIRST[::-1]:
            part_copy(d).wait_recv()
            total = total + pr[d].astype(F32)
        ys[...] = total.astype(BF16)
        for d in (2, 1, 3):
            y_copy(d).start()
        for d in (1, 3, 2):
            y_copy(d).wait_recv()
            total = total + yr[d - 1].astype(F32)
        dfull[piece(0), :] = (total * (1.0 / (8.0 * 2 * NX * NY * NZ))).astype(BF16)
        for d in FAR_FIRST:
            full_copy(d).start()
        bulk_wait(Q, 2 * Q)
        tile(2, 128, 128, far_energy)
        bulk_wait(2 * Q, 3 * Q)
        tile(2, 256, 128, far_energy)
        gamma(2, 0, LAST, w2)
        for dx in x_order:
            for dz in (0, 1, 7, 2, 6, 3, 5, 4):
                if dx or dz:
                    full_arrival(dx * NZ + dz).wait_recv()
            fw_copy(dx).start()
        bulk_wait(3 * Q, CHUNKS)
        tile(2, LAST, 128, far_energy)
        gamma_last(LAST, 128, w2)

    en1.wait_send()
    en2.wait_send()
    pair.wait_send()

    @pl.loop(0, CHUNKS)
    def _(i):
        bulk(i).wait_send()

    @pl.when(late)
    def _():
        dl.wait_send()
        for d in range(1, NY):
            y_copy(d).wait_send()
        for d in range(1, NX * NZ):
            full_copy(d).wait_send()
        for d in range(NX):
            fw_copy(d).wait_send()

    @pl.when(early)
    def _():
        for d in range(NX * NZ):
            part_copy(d).wait_send()


def finish(b, d, g, aux, lag, full, stage, aux_sem, lag_sem):
    out = pltpu.make_async_copy(g, aux, aux_sem)
    out.start()
    A = b.shape[1]
    width = A // lag_sem.shape[0]

    def copy(p):
        c = pl.ds(pl.multiple_of(p * width, 128), width)
        return pltpu.make_async_copy(stage.at[:, c], lag.at[:, c], lag_sem.at[p])

    n = d.shape[0] // NX
    for i in range(NX):
        rows = slice(i * n, (i + 1) * n)
        for k in range(NX - 1):
            j = (i + k) % NX
            full[rows, j * n : (j + 1) * n] = d[rows, k * n : (k + 1) * n]
        j = (i + NX - 1) % NX
        full[rows, j * n : (j + 1) * n] = d[j * n : (j + 1) * n, n : 2 * n].astype(F32).T.astype(BF16)

    @pl.loop(0, A // width)
    def _(p):
        c = pl.ds(pl.multiple_of(p * width, 128), width)
        stage[:, c] = nn(full[...], b[:, c]).astype(BF16)
        copy(p).start()

    @pl.loop(0, A // width)
    def _(p):
        copy(p).wait()

    out.wait()


def per_device(factors, occ_energy, vir_energy, pair_code, pair_count):
    _, V, A = factors.shape
    table = jnp.concatenate(
        [
            jnp.broadcast_to(vir_energy.astype(F32)[None, :], (8, V)),
            jnp.broadcast_to(occ_energy.astype(F32)[:, None], (8, V)),
        ]
    )
    dma = pltpu.SemaphoreType.DMA
    vmem, smem = pl.BlockSpec(memory_space=pltpu.VMEM), pl.BlockSpec(memory_space=pltpu.SMEM)
    W = V - V // NX
    rz, plane = V // NX // NZ, NX * NZ - 1
    flops = 2 * V * V * A * 7
    gamma, density = pl.pallas_call(
        body,
        out_shape=[jax.ShapeDtypeStruct((V, A), BF16), jax.ShapeDtypeStruct((V, W), BF16)],
        in_specs=[pl.BlockSpec(memory_space=pltpu.HBM), vmem, smem, smem],
        out_specs=[vmem, vmem],
        scratch_shapes=[
            pltpu.VMEM((V, A), BF16),
            pltpu.VMEM((2, V, A), BF16),
            pltpu.VMEM((3, V, V), BF16),
            pltpu.VMEM((2, 8, V), F32),
            pltpu.VMEM((V, V), F32),
            pltpu.VMEM((V, A), F32),
            pltpu.VMEM((V, V), F32),
            pltpu.VMEM((V, V), BF16),
            pltpu.VMEM((V, V), BF16),
            pltpu.VMEM((V, W), BF16),
            pltpu.VMEM((NX * NZ, rz, W), BF16),
            pltpu.VMEM((rz, W), BF16),
            pltpu.VMEM((NY - 1, rz, W), BF16),
            dma, dma, dma, dma((CHUNKS,)), dma((CHUNKS,)), dma((2,)), dma((2,)), dma, dma,
            dma((NX * NZ,)), dma((NX * NZ,)), dma((NY - 1,)), dma((NY - 1,)),
            dma((plane,)), dma((plane,)), dma((NX,)), dma((NX,)),
            pltpu.SemaphoreType.REGULAR,
        ],
        compiler_params=pltpu.CompilerParams(
            collective_id=0, has_side_effects=True, vmem_limit_bytes=36 * 2**20
        ),
        cost_estimate=pl.CostEstimate(flops=flops, bytes_accessed=8 * V * A, transcendentals=0),
        name="window",
    )(
        pltpu.with_memory_space_constraint(factors.reshape(V, A), pltpu.HBM),
        table,
        pltpu.with_memory_space_constraint(jnp.transpose(pair_code, (2, 0, 1)), pltpu.HBM),
        pltpu.with_memory_space_constraint(pair_count, pltpu.HBM),
    )
    anywhere = pl.BlockSpec(memory_space=pltpu.HBM)
    aux, lag = pl.pallas_call(
        finish,
        out_shape=[jax.ShapeDtypeStruct((V, A), BF16)] * 2,
        in_specs=[vmem, vmem, vmem],
        out_specs=[anywhere, anywhere],
        scratch_shapes=[pltpu.VMEM((V, V), BF16), pltpu.VMEM((V, A), BF16), dma, dma((STEPS,))],
        compiler_params=pltpu.CompilerParams(vmem_limit_bytes=16 * 2**20),
        cost_estimate=pl.CostEstimate(flops=2 * V * V * A, bytes_accessed=8 * V * A, transcendentals=0),
        name="finish",
    )(factors.reshape(V, A), density, gamma)
    return aux.reshape(1, V, A), lag.reshape(1, V, A)


def solution(mesh):
    in_specs = (
        P(("grp", "mem"), None, None),
        P(("grp", "mem")),
        P(),
        P("grp", None, None),
        P("grp", None),
    )
    out_specs = (P(("grp", "mem"), None, None), P(("grp", "mem"), None, None))
    return jax.shard_map(
        per_device, mesh=mesh, in_specs=in_specs, out_specs=out_specs, check_vma=False
    )
```
